32 devices in a mesh: dp: 2 (over y), seq: 16 (over z, x, core).
Axes of the slice: x: 2, y: 2, z: 4, core: 2. Of those that a mesh axis runs over, the one named last changes fastest.
Arguments:
- tokens: bfloat16 [2, 8192, 1024], P('dp', 'seq'), may hold values from -18 to 18
- lengths: int32 [2, 64], P('dp'), may hold values from 1 to 128
- w_query: bfloat16 [1024, 512], replicated, may hold values from -0.1875 to 0.1875
- w_key: bfloat16 [1024, 512], replicated, may hold values from -0.1875 to 0.1875
- w_value: bfloat16 [1024, 512], replicated, may hold values from -0.1875 to 0.1875
- w_out: bfloat16 [512, 1024], replicated, may hold values from -2 to 2
- cotangent: bfloat16 [2, 8192, 1024], P('dp', 'seq'), may hold values from -6 to 6
Outputs:
- mixed: bfloat16 [2, 8192, 1024], P('dp', 'seq')
- grad_tokens: bfloat16 [2, 8192, 1024], P('dp', 'seq')
- grad_query: float32 [1024, 512], replicated
- grad_key: float32 [1024, 512], replicated
- grad_value: float32 [1024, 512], replicated
- grad_output: float32 [512, 1024], replicated
The draws below stay inside these ranges and needn't reach their ends.
All inputs are finite; a program needn't handle non-finite values.
Results may differ from the reference program's by a relative error of at most 0.014.
The reference program's roundings to bfloat16 on the way count: a program that leaves them out, or rounds other values in their place, can miss the bound.
Values may be sent and summed in bfloat16 or wider, within the bound.
No kernel may reach another device: no remote copies, remote signals or barrier semaphores. Data moves between devices by JAX's collectives and lax.ppermute only.
A program may use at most 192 MiB of HBM per device.

```python
import math
import jax
import jax.numpy as jnp
from jax import lax

D = 1024
HEADS = 4
TILE = 128
NBARS = 64
LENGTH = 8192
SEQS = 2
HD = 512


def draw_tokens(key, part):
    base_draw = jax.random.normal(jax.random.fold_in(key, 11), (SEQS, LENGTH, D), jnp.float32)
    base_draw = jnp.clip(base_draw, -4.0, 4.0)
    return base_draw.astype(jnp.bfloat16)


def with_ends(array, stream_key, least, largest):
    longest = array.shape.index(max(array.shape))
    spots = []
    for shift in (0, 1):
        where = [jax.random.randint(jax.random.fold_in(stream_key, axis), (), 0, length) for axis, length in enumerate(array.shape)]
        where[longest] = (where[longest] + shift) % array.shape[longest]
        spots.append(tuple(where))
    return array.at[spots[0]].set(least).at[spots[1]].set(largest)


def block_levels(key, dims, split, least, largest):
    def one(dim, parts):
        steps = jax.random.uniform(jax.random.fold_in(jax.random.fold_in(key, 6), dim), (parts,), jnp.float32, least / len(split), largest / len(split))
        return jnp.repeat(jnp.exp(steps), dims[dim] // parts).reshape((-1,) + (1,) * (len(dims) - dim - 1))

    factor_of = one(*split[0])
    for cut in split[1:]:
        factor_of = factor_of * one(*cut)
    return factor_of


def bell_draw(stream_key, extent, scale, bound, split=(), kind=jnp.bfloat16):
    values = jax.random.normal(stream_key, extent, jnp.float32) * scale
    if len(split) > 0:
        values = block_levels(stream_key, extent, split, -0.22, 0.18) * values
    return jnp.clip(values, min=-bound, max=bound).astype(kind)


def setup_inputs(seed: int = 0) -> dict:
    keys = jax.random.split(jax.random.key(seed), 8)
    tokens = draw_tokens(jax.random.fold_in(keys[7], 71), 0)
    lengths = with_ends(jax.random.randint(keys[1], (SEQS, NBARS), 1, TILE + 1), jax.random.fold_in(keys[1], 1), 1, TILE).astype(jnp.int32)
    w_query = bell_draw(keys[2], (D, HD), D ** -0.5, 0.1875)
    w_key = bell_draw(keys[3], (D, HD), D ** -0.5, 0.1875)
    w_value = bell_draw(keys[4], (D, HD), D ** -0.5, 0.1875)
    w_out = bell_draw(keys[5], (HD, D), (max(HD // 64, 1)) ** -0.5, 2.0)
    cotangent = bell_draw(keys[6], (SEQS, LENGTH, D), 1.0, 6.0, ((0, 2), (1, 16)))
    return {"tokens": tokens, "lengths": lengths, "w_query": w_query, "w_key": w_key, "w_value": w_value, "w_out": w_out, "cotangent": cotangent}


bar_offsets = (0, 1, 2, 4, 8, 12, 16, 24, 32)
group_bars = 4
far_score = -1e+30

def product(form, left, right):
    return jnp.einsum(form, left.astype(jnp.float32), right.astype(jnp.float32))

def summarize(bar_rows, length):
    slot_ids = jnp.arange(bar_rows.shape[1], dtype=jnp.int32)
    live_slots = slot_ids[None, :] < length[:, None]
    running = lax.optimization_barrier(jnp.sum(jnp.where(live_slots[:, :, None], bar_rows.astype(jnp.float32), 0.0), axis=1))
    return (running / length[:, None].astype(jnp.float32)).astype(jnp.bfloat16)

def bar_block(queries, ext_key, ext_value, ext_length, base_bar, bar_ids, query_length, summary_key, summary_value, grad_context):
    group_count, tile_len, head_count, head_dim = queries.shape
    sources = len(bar_offsets)
    key_parts = []
    value_parts = []
    length_parts = []
    for offset in bar_offsets:
        first_bar = base_bar - offset
        key_parts.append(lax.dynamic_slice_in_dim(ext_key, first_bar, group_count, 0))
        value_parts.append(lax.dynamic_slice_in_dim(ext_value, first_bar, group_count, 0))
        length_parts.append(lax.dynamic_slice_in_dim(ext_length, first_bar, group_count, 0))
    fine_key = jnp.stack(key_parts, 1).reshape(group_count, sources * tile_len, head_count, head_dim)
    fine_value = jnp.stack(value_parts, 1).reshape(group_count, sources * tile_len, head_count, head_dim)
    fine_length = jnp.stack(length_parts, 1)
    slot_ids = jnp.arange(tile_len, dtype=jnp.int32)
    key_live = slot_ids[None, None, :] < fine_length[:, :, None]
    causal = slot_ids[None, :] <= slot_ids[:, None]
    other_bar = jnp.arange(sources, dtype=jnp.int32) != 0
    fine_live = key_live[:, None, :, :] & (causal[None, :, None, :] | other_bar[None, None, :, None])
    fine_live = fine_live.reshape(group_count, 1, tile_len, sources * tile_len)
    distance = bar_ids[:, None] - jnp.arange(summary_key.shape[0], dtype=jnp.int32)[None, :]
    coarse_live = distance >= 1
    for offset in bar_offsets[1:]:
        coarse_live = coarse_live & (distance != offset)
    coarse_live = coarse_live[:, None, None, :]
    score_scale = 1.0 / math.sqrt(head_dim)
    fine_score = product('gqhe,gkhe->ghqk', queries, fine_key) * score_scale
    coarse_score = product('gqhe,nhe->ghqn', queries, summary_key) * score_scale
    fine_score = jnp.where(fine_live, fine_score, far_score)
    coarse_score = jnp.where(coarse_live, coarse_score, far_score)
    top_score = jnp.maximum(lax.optimization_barrier(jnp.max(fine_score, axis=-1)), lax.optimization_barrier(jnp.max(coarse_score, axis=-1)))[..., None]
    fine_exp = jnp.where(fine_live, jnp.exp(fine_score - top_score), 0.0)
    coarse_exp = jnp.where(coarse_live, jnp.exp(coarse_score - top_score), 0.0)
    denominator = (lax.optimization_barrier(jnp.sum(fine_exp, axis=-1)) + lax.optimization_barrier(jnp.sum(coarse_exp, axis=-1)))[..., None]
    fine_prob = fine_exp / denominator
    coarse_prob = coarse_exp / denominator
    fine_round = fine_prob.astype(jnp.bfloat16)
    coarse_round = coarse_prob.astype(jnp.bfloat16)
    attended_context = product('ghqk,gkhe->gqhe', fine_round, fine_value) + product('ghqn,nhe->gqhe', coarse_round, summary_value)
    query_live = slot_ids[None, :] < query_length[:, None]
    attended_context = jnp.where(query_live[:, :, None, None], attended_context, 0.0)
    fine_dp = product('gqhe,gkhe->ghqk', grad_context, fine_value)
    coarse_dp = product('gqhe,nhe->ghqn', grad_context, summary_value)
    delta = (lax.optimization_barrier(jnp.sum(fine_prob * fine_dp, axis=-1)) + lax.optimization_barrier(jnp.sum(coarse_prob * coarse_dp, axis=-1)))[..., None]
    fine_ds = (fine_prob * (fine_dp - delta) * score_scale).astype(jnp.bfloat16)
    coarse_ds = (coarse_prob * (coarse_dp - delta) * score_scale).astype(jnp.bfloat16)
    query_gradient_rows = product('ghqk,gkhe->gqhe', fine_ds, fine_key) + product('ghqn,nhe->gqhe', coarse_ds, summary_key)
    fine_gk = product('ghqk,gqhe->gkhe', fine_ds, queries).reshape(group_count, sources, tile_len, head_count, head_dim)
    fine_gv = product('ghqk,gqhe->gkhe', fine_round, grad_context).reshape(group_count, sources, tile_len, head_count, head_dim)
    coarse_key_gradient = product('ghqn,gqhe->nhe', coarse_ds, queries)
    coarse_value_gradient = product('ghqn,gqhe->nhe', coarse_round, grad_context)
    return (attended_context, query_gradient_rows, fine_gk, fine_gv, coarse_key_gradient, coarse_value_gradient)

def spread(running, grads, base_bar):
    group_count = grads.shape[0]
    for position, offset in enumerate(bar_offsets):
        first_bar = base_bar - offset
        current = lax.dynamic_slice_in_dim(running, first_bar, group_count, 0)
        running = lax.dynamic_update_slice_in_dim(running, current + grads[:, position], first_bar, 0)
    return running

def reference(tokens, lengths, w_query, w_key, w_value, w_out, cotangent):
    inner_width = w_query.shape[1]
    head_dim = inner_width // HEADS
    pad_bars = bar_offsets[-1]
    bar_grand_total = lengths.shape[1]
    grad_q_sum = jnp.zeros(w_query.shape, jnp.float32)
    grad_k_sum = jnp.zeros(w_query.shape, jnp.float32)
    grad_v_sum = jnp.zeros(w_query.shape, jnp.float32)
    grad_o_sum = jnp.zeros(w_out.shape, jnp.float32)
    mixed_rows = []
    grad_rows = []
    for seq_row in range(tokens.shape[0]):
        inputs = tokens[seq_row]
        grad_out = cotangent[seq_row]
        length = lengths[seq_row]
        queries = jnp.dot(inputs, w_query, preferred_element_type=jnp.float32).astype(jnp.bfloat16)
        keys_all = jnp.dot(inputs, w_key, preferred_element_type=jnp.float32).astype(jnp.bfloat16)
        values_all = jnp.dot(inputs, w_value, preferred_element_type=jnp.float32).astype(jnp.bfloat16)
        key_bars = keys_all.reshape(bar_grand_total, TILE, inner_width)
        value_bars = values_all.reshape(bar_grand_total, TILE, inner_width)
        summary_key = summarize(key_bars, length).reshape(bar_grand_total, HEADS, head_dim)
        summary_value = summarize(value_bars, length).reshape(bar_grand_total, HEADS, head_dim)
        slot_ids = jnp.arange(TILE, dtype=jnp.int32)
        live_slots = slot_ids[None, :] < length[:, None]
        token_live = live_slots.reshape(-1)
        grad_context = product('td,ed->te', grad_out, w_out)
        grad_context = jnp.where(token_live[:, None], grad_context, 0.0).astype(jnp.bfloat16)
        zero_bars = jnp.zeros((pad_bars, TILE, HEADS, head_dim), jnp.bfloat16)
        ext_key = jnp.concatenate([zero_bars, keys_all.reshape(bar_grand_total, TILE, HEADS, head_dim)], 0)
        ext_value = jnp.concatenate([zero_bars, values_all.reshape(bar_grand_total, TILE, HEADS, head_dim)], 0)
        ext_length = jnp.concatenate([jnp.zeros((pad_bars,), jnp.int32), length], 0)
        query_bars = queries.reshape(bar_grand_total, TILE, HEADS, head_dim)
        grad_bars = grad_context.reshape(bar_grand_total, TILE, HEADS, head_dim)

        def step(carried_state, block_index):
            accumulated_key, accumulated_value, accumulated_summary_key, accumulated_summary_value = carried_state
            begin_bar = (block_index * group_bars).astype(jnp.int32)
            query_block = lax.dynamic_slice_in_dim(query_bars, begin_bar, group_bars, 0)
            grad_block = lax.dynamic_slice_in_dim(grad_bars, begin_bar, group_bars, 0)
            length_block = lax.dynamic_slice_in_dim(length, begin_bar, group_bars, 0)
            base_bar = (pad_bars + begin_bar).astype(jnp.int32)
            bar_ids = begin_bar + jnp.arange(group_bars, dtype=jnp.int32)
            result = bar_block(query_block, ext_key, ext_value, ext_length, base_bar, bar_ids, length_block, summary_key, summary_value, grad_block)
            attended_context, query_gradient_rows, fine_gk, fine_gv, coarse_key_gradient, coarse_value_gradient = result
            accumulated_key = spread(accumulated_key, fine_gk, base_bar)
            accumulated_value = spread(accumulated_value, fine_gv, base_bar)
            return ((accumulated_key, accumulated_value, accumulated_summary_key + coarse_key_gradient, accumulated_summary_value + coarse_value_gradient), (attended_context.astype(jnp.bfloat16), query_gradient_rows.astype(jnp.bfloat16)))
        ext_zero = jnp.zeros((pad_bars + bar_grand_total, TILE, HEADS, head_dim), jnp.float32)
        sum_zero = jnp.zeros((bar_grand_total, HEADS, head_dim), jnp.float32)
        carried_state, stacked = lax.scan(step, (ext_zero, ext_zero, sum_zero, sum_zero), jnp.arange(bar_grand_total // group_bars, dtype=jnp.int32))
        accumulated_key, accumulated_value, accumulated_summary_key, accumulated_summary_value = carried_state
        attended_context = stacked[0].reshape(-1, inner_width)
        query_gradient_rows = stacked[1].reshape(-1, inner_width)
        inverse_denominator = 1.0 / length.astype(jnp.float32)
        shared_key_rows = accumulated_summary_key.reshape(bar_grand_total, inner_width) * inverse_denominator[:, None]
        share_value = accumulated_summary_value.reshape(bar_grand_total, inner_width) * inverse_denominator[:, None]
        own_key = accumulated_key[pad_bars:].reshape(bar_grand_total, TILE, inner_width) + jnp.where(live_slots[:, :, None], shared_key_rows[:, None, :], 0.0)
        own_value = accumulated_value[pad_bars:].reshape(bar_grand_total, TILE, inner_width) + jnp.where(live_slots[:, :, None], share_value[:, None, :], 0.0)
        grad_keys = own_key.reshape(-1, inner_width).astype(jnp.bfloat16)
        grad_values = own_value.reshape(-1, inner_width).astype(jnp.bfloat16)
        mixed_rows.append(jnp.dot(attended_context, w_out, preferred_element_type=jnp.float32).astype(jnp.bfloat16))
        grad_in = product('te,de->td', query_gradient_rows, w_query) + product('te,de->td', grad_keys, w_key) + product('te,de->td', grad_values, w_value)
        grad_rows.append(grad_in.astype(jnp.bfloat16))
        grad_q_sum = grad_q_sum + product('td,te->de', inputs, query_gradient_rows)
        grad_k_sum = grad_k_sum + product('td,te->de', inputs, grad_keys)
        grad_v_sum = grad_v_sum + product('td,te->de', inputs, grad_values)
        grad_o_sum = grad_o_sum + product('te,td->ed', attended_context, grad_out)
    return (jnp.stack(mixed_rows, 0), jnp.stack(grad_rows, 0), grad_q_sum, grad_k_sum, grad_v_sum, grad_o_sum)
```

```python
import functools
import math

import jax
import jax.numpy as jnp
from jax import lax
from jax.experimental import pallas as pl
from jax.experimental.pallas import tpu as pltpu
from jax.sharding import PartitionSpec as P

HEADS = 4
TILE = 128

bar_offsets = (0, 1, 2, 4, 8, 12, 16, 24, 32)
far_score = -1e30

BF = jnp.bfloat16
F32 = jnp.float32
NT = (((1,), (1,)), ((), ()))
NN = (((1,), (0,)), ((), ()))
VM = pl.BlockSpec(memory_space=pltpu.VMEM)
SM = pl.BlockSpec(memory_space=pltpu.SMEM)


def dot(a, b, dims=NN):
    return lax.dot_general(a, b, dims, preferred_element_type=F32)


def swap(block, axis, mask):
    return lax.ppermute(block, axis, [(i, i ^ mask) for i in range(lax.axis_size(axis))])


def shifted(block, axis, distance):
    devices = range(lax.axis_size(axis))
    return lax.ppermute(block, axis, [(i - distance, i) for i in devices if i - distance in devices])


def call(kernel, outs, operands, specs, name, flops, moved, scratch=()):
    return pl.pallas_call(
        kernel,
        out_shape=outs,
        in_specs=specs,
        out_specs=[VM] * len(outs),
        scratch_shapes=list(scratch),
        compiler_params=pltpu.CompilerParams(vmem_limit_bytes=56 * 1024 * 1024),
        cost_estimate=pl.CostEstimate(flops=flops, bytes_accessed=moved, transcendentals=0),
        name=name,
    )(*operands)


def column(h):
    return pl.ds(pl.multiple_of(h * TILE, TILE), TILE)


def kv_kernel(rank_ref, x_ref, wk_ref, wv_ref, *outs):
    x = x_ref[...]
    for j, out in enumerate(outs):
        h = jnp.bitwise_xor(rank_ref[0], j)
        w = jnp.concatenate([wk_ref[:, column(h)], wv_ref[:, column(h)]], axis=1)
        out[...] = dot(x, w).astype(BF)


def qg_kernel(rank_ref, len_ref, x_ref, c_ref, wq_ref, wo_ref, *outs):
    x = x_ref[...]
    c = c_ref[...]
    rows = x.shape[0]
    slot = lax.broadcasted_iota(jnp.int32, (TILE, TILE), 0)
    for j, out in enumerate(outs):
        h = jnp.bitwise_xor(rank_ref[0], j)
        out[:, :TILE] = dot(x, wq_ref[:, column(h)]).astype(BF)
        g = dot(c, wo_ref[column(h), :], NT)
        for b in range(rows // TILE):
            live = slot < len_ref[b]
            part = g[b * TILE : (b + 1) * TILE]
            out[b * TILE : (b + 1) * TILE, TILE:] = jnp.where(live, part, 0.0).astype(BF)


def summary_kernel(rank_ref, len_ref, *refs):
    blocks, out = refs[:-1], refs[-1]
    bars = blocks[0].shape[0] // TILE
    slot = lax.broadcasted_iota(jnp.int32, (TILE, 2 * TILE), 0)
    for j, block in enumerate(blocks):
        first = jnp.bitwise_xor(rank_ref[0], j) * bars
        for b in range(bars):
            length = len_ref[first + b]
            rows = block[b * TILE : (b + 1) * TILE, :].astype(F32)
            total = jnp.sum(jnp.where(slot < length, rows, 0.0), axis=0, keepdims=True)
            count = jnp.full((1, 2 * TILE), length, jnp.int32).astype(F32)
            out[pl.ds(first + b, 1), :] = total / count


def attention_kernel(reach, groups, rank_ref, len_ref, qg_in, kv_in, sum_in, outs, scratch):
    qg, kv, kvt, acc, sc, dpc, pd, w2, xo, sumt, gsum = scratch
    xo_out, own_out, back_out, gs_out = outs
    block_rows = qg_in[0].shape[0]
    bars = block_rows // TILE
    span = bars * HEADS
    rank = rank_ref[0]
    first_row = rank_ref[1]
    n_coarse = sum_in.shape[0]
    slots = len(bar_offsets)
    c_slots = n_coarse // TILE
    scale = 1.0 / math.sqrt(TILE)
    c2 = scale * math.log2(math.e)

    def place(j):
        return jnp.bitwise_xor(rank, j) * block_rows

    def rows_at(start, size):
        return pl.ds(pl.multiple_of(start, TILE), size)

    for j in range(HEADS):
        qg[rows_at(place(j), block_rows), :] = qg_in[j][...]
        for t in range(reach + 1):
            base = (reach - t) * span * TILE
            kv[rows_at(base + place(j), block_rows), :] = kv_in[t][j][...]
    acc[...] = jnp.zeros_like(acc)
    gsum[...] = jnp.zeros_like(gsum)
    w2[...] = jnp.zeros_like(w2)
    sumt[...] = sum_in[...].T

    def turn(b, carry):
        kvt[b] = kv[rows_at(b * TILE, TILE), :].T
        return carry

    lax.fori_loop(0, (reach + 1) * span, turn, 0)

    key_slot = lax.broadcasted_iota(jnp.int32, (TILE, TILE), 0)
    query_slot = lax.broadcasted_iota(jnp.int32, (TILE, TILE), 1)

    def bar(i, carry):
        e = reach * span + i
        own = rows_at(i * TILE, TILE)
        w2[:TILE, :TILE] = qg[own, :TILE]
        w2[TILE:, TILE:] = qg[own, TILE:]
        w = w2[...]
        top = None
        for s in range(slots + c_slots):
            if s < slots:
                sd = dot(kv[rows_at((e - bar_offsets[s]) * TILE, TILE), :], w, NT)
                live = key_slot < len_ref[e - bar_offsets[s]]
                if bar_offsets[s] == 0:
                    live = live & (key_slot <= query_slot)
            else:
                c = s - slots
                sd = dot(sum_in[c * TILE : (c + 1) * TILE, :], w, NT)
                row = key_slot + c * TILE
                distance = i + (n_coarse - span) - row
                live = (distance >= 1) & (row >= first_row)
                for offset in bar_offsets[1:]:
                    live = live & (distance != offset)
            score = jnp.where(live, sd[:, :TILE], far_score)
            sc[s * TILE : (s + 1) * TILE, :] = score
            dpc[s * TILE : (s + 1) * TILE, :] = sd[:, TILE:]
            top = score if top is None else jnp.maximum(top, score)
        top = jnp.max(top, axis=0, keepdims=True) * c2
        total = jnp.zeros((TILE, TILE), F32)
        weighted = jnp.zeros((TILE, TILE), F32)
        for s in range(slots + c_slots):
            at = slice(s * TILE, (s + 1) * TILE)
            p = jnp.exp2(sc[at, :] * c2 - top)
            sc[at, :] = p
            total = total + p
            weighted = weighted + p * dpc[at, :]
        inverse = 1.0 / jnp.sum(total, axis=0, keepdims=True)
        delta = jnp.sum(weighted, axis=0, keepdims=True) * inverse
        for s in range(slots + c_slots):
            at = slice(s * TILE, (s + 1) * TILE)
            p = sc[at, :] * inverse
            pd[at, TILE:] = p.astype(BF)
            pd[at, :TILE] = (p * (dpc[at, :] - delta) * scale).astype(BF)
        for s in range(slots):
            at = rows_at((e - bar_offsets[s]) * TILE, TILE)
            acc[at, :] = acc[at, :] + dot(pd[s * TILE : (s + 1) * TILE, :], w)
        gsum[...] = gsum[...] + dot(pd[slots * TILE :, :], w)

        def turned(s, half):
            if s < slots:
                return kvt[e - bar_offsets[s], half]
            return sumt[half, (s - slots) * TILE : (s - slots + 1) * TILE]

        low, high = slice(0, TILE), slice(TILE, 2 * TILE)
        context = jnp.zeros((TILE, TILE), F32)
        gq = jnp.zeros((TILE, TILE), F32)
        for s in range(0, slots + c_slots, 2):
            many = [k for k in (s, s + 1) if k < slots + c_slots]
            at = slice(s * TILE, (s + len(many)) * TILE)
            values = jnp.concatenate([turned(k, high) for k in many], axis=1)
            keys = jnp.concatenate([turned(k, low) for k in many], axis=1)
            context = context + dot(values, pd[at, TILE:])
            gq = gq + dot(keys, pd[at, :TILE])
        context = jnp.where(query_slot < len_ref[e], context, 0.0)
        xo[own, :TILE] = context.T.astype(BF)
        xo[own, TILE:] = gq.T.astype(BF)
        return carry

    lax.fori_loop(0, span, bar, 0)
    for j in range(HEADS):
        xo_out[j][...] = xo[rows_at(place(j), block_rows), :]
        own_out[j][...] = acc[rows_at(reach * span * TILE + place(j), block_rows), :]
        for t in range(1, reach + 1):
            part = acc[rows_at((reach - t) * span * TILE + place(j), block_rows), :]
            back_out[t - 1][j][...] = part.astype(back_out[t - 1][j].dtype)
    gs_out[...] = gsum[...]


def assemble_kernel(rank_ref, *refs):
    blocks, outs = refs[:HEADS], refs[HEADS:]
    for j, block in enumerate(blocks):
        h = jnp.bitwise_xor(rank_ref[0], j)
        outs[0][:, column(h)] = block[:, :TILE]
        outs[1][:, column(h)] = block[:, TILE:]


def finish_kernel(groups, rank_ref, len_ref, *refs):
    owns, backs = refs[:HEADS], refs[HEADS : 2 * HEADS]
    sums, outs = refs[2 * HEADS : -HEADS - 1], refs[-HEADS - 1 : -1]
    tot = refs[-1]
    total = sums[0][...]
    for part in sums[1:]:
        total = total + part[...]
    tot[...] = total
    bars = owns[0].shape[0] // TILE
    slot = lax.broadcasted_iota(jnp.int32, (TILE, 2 * TILE), 0)
    for j in range(HEADS):
        first = jnp.bitwise_xor(rank_ref[0], j) * bars
        for b in range(bars):
            at = slice(b * TILE, (b + 1) * TILE)
            length = len_ref[first + b]
            count = jnp.full((1, 2 * TILE), length, jnp.int32).astype(F32)
            share = tot[pl.ds(first + b, 1), :] * (1.0 / count)
            value = owns[j][at, :] + backs[j][at, :].astype(F32)
            outs[j][at, :] = (value + jnp.where(slot < length, share, 0.0)).astype(BF)


def all_reduce(part, steps):
    for axis, mask in steps:
        bit = (lax.axis_index(axis) // mask) % 2
        half = part.shape[0] // 2
        keep = lax.dynamic_slice_in_dim(part, bit * half, half, 0)
        send = lax.dynamic_slice_in_dim(part, (1 - bit) * half, half, 0)
        got = swap(send, axis, mask)
        part = (keep.astype(F32) + got.astype(F32)).astype(BF)
    for axis, mask in reversed(steps):
        bit = (lax.axis_index(axis) // mask) % 2
        got = swap(part, axis, mask)
        part = jnp.concatenate(
            [jnp.where(bit == 0, part, got), jnp.where(bit == 0, got, part)], 0
        )
    return part


def local(tokens, lengths, w_query, w_key, w_value, w_out, cotangent):
    inputs = tokens[0]
    grad_out = cotangent[0]
    rows, width = inputs.shape
    inner = w_query.shape[1]
    bars = rows // TILE
    span = HEADS * bars
    seq_size = lax.axis_size("seq")
    groups = seq_size // HEADS
    reach = -(-bar_offsets[-1] // span)
    index = lax.axis_index("seq")
    rank = index % HEADS
    group = index // HEADS
    all_length = lengths[0]
    own_length = lax.dynamic_slice_in_dim(all_length, index * bars, bars, 0)
    group_length = lax.dynamic_slice_in_dim(all_length, group * span, span, 0)
    padded = jnp.concatenate([jnp.zeros((reach * span,), jnp.int32), all_length], 0)
    ext_length = lax.dynamic_slice_in_dim(padded, group * span, (reach + 1) * span, 0)
    n_coarse = -(-(groups * span) // TILE) * TILE
    rank_info = jnp.stack([rank, n_coarse - span - group * span]).astype(jnp.int32)

    pair = 2 * TILE
    block = jax.ShapeDtypeStruct((rows, pair), BF)
    wide = jax.ShapeDtypeStruct((rows, pair), F32)
    project = 2 * rows * width * inner

    kv = call(
        kv_kernel,
        [block] * HEADS,
        (rank_info, inputs, w_key, w_value),
        [SM, VM, VM, VM],
        "project_kv",
        2 * project,
        6 << 20,
    )
    kv_own = [kv[0]] + [swap(kv[j], "seq", j) for j in range(1, HEADS)]
    kv_all = [kv_own]
    for _ in range(reach):
        kv_all.append([shifted(b, "seq", HEADS) for b in kv_all[-1]])
    qg = call(
        qg_kernel,
        [block] * HEADS,
        (rank_info, own_length, inputs, grad_out, w_query, w_out),
        [SM, SM, VM, VM, VM, VM],
        "project_qg",
        2 * project,
        6 << 20,
    )
    qg = [qg[0]] + [swap(qg[j], "seq", j) for j in range(1, HEADS)]
    summary = call(
        summary_kernel,
        [jax.ShapeDtypeStruct((span, pair), F32)],
        (rank_info, group_length, *kv_own),
        [SM, SM] + [VM] * HEADS,
        "summaries",
        1 << 20,
        1 << 20,
    )[0].astype(BF)
    far = [shifted(summary, "seq", HEADS * t) for t in range(1, groups)]
    padding = jnp.zeros((n_coarse - groups * span, pair), BF)
    sums = jnp.concatenate([padding] + far[::-1] + [summary], 0)

    ext_rows = (reach + 1) * span * TILE
    slots = len(bar_offsets) * TILE + n_coarse
    outs = (
        [block] * HEADS
        + [wide] * HEADS
        + [wide] * (HEADS * (reach - 1))
        + [block] * HEADS
        + [jax.ShapeDtypeStruct((n_coarse, pair), F32)]
    )

    def kernel(rank_ref, len_ref, *refs):
        take = iter(refs)
        get = lambda n: [next(take) for _ in range(n)]
        qg_in = get(HEADS)
        kv_in = [get(HEADS) for _ in range(reach + 1)]
        sum_in = next(take)
        xo_out, own_out = get(HEADS), get(HEADS)
        back_out = [get(HEADS) for _ in range(reach)]
        gs_out = next(take)
        attention_kernel(
            reach, groups, rank_ref, len_ref, qg_in, kv_in, sum_in,
            (xo_out, own_out, back_out, gs_out), list(take),
        )

    result = call(
        kernel,
        outs,
        (rank_info, ext_length, *qg, *[b for level in kv_all for b in level], sums),
        [SM, SM] + [VM] * (HEADS * (reach + 2) + 1),
        "attention",
        16 * slots * TILE * TILE * span,
        16 << 20,
        (
            pltpu.VMEM((span * TILE, pair), BF),
            pltpu.VMEM((ext_rows, pair), BF),
            pltpu.VMEM(((reach + 1) * span, pair, TILE), BF),
            pltpu.VMEM((ext_rows, pair), F32),
            pltpu.VMEM((slots, TILE), F32),
            pltpu.VMEM((slots, TILE), F32),
            pltpu.VMEM((slots, pair), BF),
            pltpu.VMEM((pair, pair), BF),
            pltpu.VMEM((span * TILE, pair), BF),
            pltpu.VMEM((pair, n_coarse), BF),
            pltpu.VMEM((n_coarse, pair), F32),
        ),
    )
    take = iter(result)
    get = lambda n: [next(take) for _ in range(n)]
    xo, own = get(HEADS), get(HEADS)
    back = [get(HEADS) for _ in range(reach)]
    gs = next(take)

    carry = back[reach - 1]
    for t in range(reach - 1, -1, -1):
        got = [shifted(b, "seq", -HEADS) for b in carry]
        if t > 0:
            carry = [(b + g.astype(F32)).astype(BF) for b, g in zip(back[t - 1], got)]
    gs_parts = [gs[n_coarse - span :]]
    for t in range(1, groups):
        part = gs[n_coarse - (t + 1) * span : n_coarse - t * span]
        gs_parts.append(shifted(part, "seq", -HEADS * t))

    xo = [xo[0]] + [swap(xo[j], "seq", j) for j in range(1, HEADS)]
    full = jax.ShapeDtypeStruct((rows, inner), BF)
    context, gq = call(
        assemble_kernel, [full] * 2, (rank_info, *xo), [SM] + [VM] * HEADS, "join_q", 1 << 20, 2 << 20
    )
    gkv = call(
        functools.partial(finish_kernel, groups),
        [block] * HEADS,
        (rank_info, group_length, *own, *got, *gs_parts),
        [SM, SM] + [VM] * (2 * HEADS + groups),
        "finish_kv",
        1 << 20,
        4 << 20,
        (pltpu.VMEM((span, pair), F32),),
    )
    gkv = [gkv[0]] + [swap(gkv[j], "seq", j) for j in range(1, HEADS)]
    gk, gv = call(
        assemble_kernel, [full] * 2, (rank_info, *gkv), [SM] + [VM] * HEADS, "join_kv", 1 << 20, 2 << 20
    )

    mixed = dot(context, w_out).astype(BF)
    steps = [("seq", 1)]
    steps += [("dp", 1 << b) for b in range(lax.axis_size("dp").bit_length() - 1)]
    steps += [("seq", 1 << b) for b in range(1, seq_size.bit_length() - 1)]
    tn = (((0,), (0,)), ((), ()))
    grad_o = dot(grad_out, context, tn).astype(BF)
    grad_q = dot(inputs, gq, tn).astype(BF)
    first = all_reduce(jnp.concatenate([grad_o, grad_q], 1), steps)
    grad_k = dot(inputs, gk, tn).astype(BF)
    grad_v = dot(inputs, gv, tn).astype(BF)
    second = all_reduce(jnp.concatenate([grad_k, grad_v], 1), steps)
    grad_in = dot(gq, w_query, NT) + dot(gk, w_key, NT) + dot(gv, w_value, NT)
    return (
        mixed[None],
        grad_in.astype(BF)[None],
        first[:, inner:].astype(F32),
        second[:, :inner].astype(F32),
        second[:, inner:].astype(F32),
        first[:, :inner].astype(F32).T,
    )


def solution(mesh):
    placed = (P("dp", "seq", None), P("dp", None), P(), P(), P(), P(), P("dp", "seq", None))
    return jax.shard_map(
        local,
        mesh=mesh,
        in_specs=placed,
        out_specs=(P("dp", "seq", None), P("dp", "seq", None), P(), P(), P(), P()),
        check_vma=False,
    )
```

```python
import functools
import math

import jax
import jax.numpy as jnp
from jax import lax
from jax.experimental import pallas as pl
from jax.experimental.pallas import tpu as pltpu
from jax.sharding import PartitionSpec as P

HEADS = 4
TILE = 128

bar_offsets = (0, 1, 2, 4, 8, 12, 16, 24, 32)
far_score = -1e30

BF = jnp.bfloat16
F32 = jnp.float32
NT = (((1,), (1,)), ((), ()))
NN = (((1,), (0,)), ((), ()))
VM = pl.BlockSpec(memory_space=pltpu.VMEM)
SM = pl.BlockSpec(memory_space=pltpu.SMEM)


def dot(a, b, dims=NN):
    return lax.dot_general(a, b, dims, preferred_element_type=F32)


def swap(block, axis, mask):
    return lax.ppermute(block, axis, [(i, i ^ mask) for i in range(lax.axis_size(axis))])


def shifted(block, axis, distance):
    devices = range(lax.axis_size(axis))
    return lax.ppermute(block, axis, [(i - distance, i) for i in devices if i - distance in devices])


def call(kernel, outs, operands, specs, name, flops, moved, scratch=()):
    return pl.pallas_call(
        kernel,
        out_shape=outs,
        in_specs=specs,
        out_specs=[VM] * len(outs),
        scratch_shapes=list(scratch),
        compiler_params=pltpu.CompilerParams(vmem_limit_bytes=56 * 1024 * 1024),
        cost_estimate=pl.CostEstimate(flops=flops, bytes_accessed=moved, transcendentals=0),
        name=name,
    )(*operands)


def column(h):
    return pl.ds(pl.multiple_of(h * TILE, TILE), TILE)


def kv_kernel(rank_ref, x_ref, wk_ref, wv_ref, *outs):
    x = x_ref[...]
    for j, out in enumerate(outs):
        h = jnp.bitwise_xor(rank_ref[0], j)
        w = jnp.concatenate([wk_ref[:, column(h)], wv_ref[:, column(h)]], axis=1)
        out[...] = dot(x, w).astype(BF)


def qg_kernel(rank_ref, len_ref, x_ref, c_ref, wq_ref, wo_ref, *outs):
    x = x_ref[...]
    c = c_ref[...]
    rows = x.shape[0]
    slot = lax.broadcasted_iota(jnp.int32, (TILE, TILE), 0)
    for j, out in enumerate(outs):
        h = jnp.bitwise_xor(rank_ref[0], j)
        out[:, :TILE] = dot(x, wq_ref[:, column(h)]).astype(BF)
        g = dot(c, wo_ref[column(h), :], NT)
        for b in range(rows // TILE):
            live = slot < len_ref[b]
            part = g[b * TILE : (b + 1) * TILE]
            out[b * TILE : (b + 1) * TILE, TILE:] = jnp.where(live, part, 0.0).astype(BF)


def summary_kernel(rank_ref, len_ref, *refs):
    blocks, out = refs[:-1], refs[-1]
    bars = blocks[0].shape[0] // TILE
    slot = lax.broadcasted_iota(jnp.int32, (TILE, 2 * TILE), 0)
    for j, block in enumerate(blocks):
        first = jnp.bitwise_xor(rank_ref[0], j) * bars
        for b in range(bars):
            length = len_ref[first + b]
            rows = block[b * TILE : (b + 1) * TILE, :].astype(F32)
            total = jnp.sum(jnp.where(slot < length, rows, 0.0), axis=0, keepdims=True)
            count = jnp.full((1, 2 * TILE), length, jnp.int32).astype(F32)
            out[pl.ds(first + b, 1), :] = total / count


def attention_kernel(reach, rank_ref, len_ref, qg_in, kv_in, sum_in, outs, scratch):
    qg, kv, kvt, acc, sc, dpc, pd, w2, xo, sumt, gsum = scratch
    xo_out, own_out, back_out, gs_out = outs
    block_rows = qg_in[0].shape[0]
    bars = block_rows // TILE
    span = bars * HEADS
    rank = rank_ref[0]
    first_row = rank_ref[1]
    n_coarse = sum_in.shape[0]
    slots = len(bar_offsets)
    c_slots = n_coarse // TILE
    scale = 1.0 / math.sqrt(TILE)
    c2 = scale * math.log2(math.e)

    def place(j):
        return jnp.bitwise_xor(rank, j) * block_rows

    def rows_at(start, size):
        return pl.ds(pl.multiple_of(start, TILE), size)

    for j in range(HEADS):
        qg[rows_at(place(j), block_rows), :] = qg_in[j][...]
        for t in range(reach + 1):
            base = (reach - t) * span * TILE
            many = len(kv_in[t])
            piece = kv_in[t][j * many // HEADS]
            start = j % (HEADS // many) * block_rows
            kv[rows_at(base + place(j), block_rows), :] = piece[start : start + block_rows, :]
    acc[...] = jnp.zeros_like(acc)
    gsum[...] = jnp.zeros_like(gsum)
    w2[...] = jnp.zeros_like(w2)
    sumt[...] = sum_in[...].T

    def turn(b, carry):
        kvt[b] = kv[rows_at(b * TILE, TILE), :].T
        return carry

    lax.fori_loop(0, (reach + 1) * span, turn, 0)

    key_slot = lax.broadcasted_iota(jnp.int32, (TILE, TILE), 0)
    query_slot = lax.broadcasted_iota(jnp.int32, (TILE, TILE), 1)

    def bar(i, carry):
        e = reach * span + i
        own = rows_at(i * TILE, TILE)
        w2[:TILE, :TILE] = qg[own, :TILE]
        w2[TILE:, TILE:] = qg[own, TILE:]
        w = w2[...]
        top = None
        for s in range(slots + c_slots):
            if s < slots:
                sd = dot(kv[rows_at((e - bar_offsets[s]) * TILE, TILE), :], w, NT)
                live = key_slot < len_ref[e - bar_offsets[s]]
                if bar_offsets[s] == 0:
                    live = live & (key_slot <= query_slot)
            else:
                c = s - slots
                sd = dot(sum_in[c * TILE : (c + 1) * TILE, :], w, NT)
                row = key_slot + c * TILE
                distance = i + (n_coarse - span) - row
                live = (distance >= 1) & (row >= first_row)
                for offset in bar_offsets[1:]:
                    live = live & (distance != offset)
            score = jnp.where(live, sd[:, :TILE], far_score)
            sc[s * TILE : (s + 1) * TILE, :] = score
            dpc[s * TILE : (s + 1) * TILE, :] = sd[:, TILE:]
            top = score if top is None else jnp.maximum(top, score)
        top = jnp.max(top, axis=0, keepdims=True) * c2
        total = jnp.zeros((TILE, TILE), F32)
        weighted = jnp.zeros((TILE, TILE), F32)
        for s in range(slots + c_slots):
            at = slice(s * TILE, (s + 1) * TILE)
            p = jnp.exp2(sc[at, :] * c2 - top)
            sc[at, :] = p
            total = total + p
            weighted = weighted + p * dpc[at, :]
        inverse = 1.0 / jnp.sum(total, axis=0, keepdims=True)
        delta = jnp.sum(weighted, axis=0, keepdims=True) * inverse
        for s in range(slots + c_slots):
            at = slice(s * TILE, (s + 1) * TILE)
            p = sc[at, :] * inverse
            pd[at, TILE:] = p.astype(BF)
            pd[at, :TILE] = (p * (dpc[at, :] - delta) * scale).astype(BF)
        for s in range(slots):
            at = rows_at((e - bar_offsets[s]) * TILE, TILE)
            acc[at, :] = acc[at, :] + dot(pd[s * TILE : (s + 1) * TILE, :], w)
        gsum[...] = gsum[...] + dot(pd[slots * TILE :, :], w)

        def turned(s, half):
            if s < slots:
                return kvt[e - bar_offsets[s], half]
            return sumt[half, (s - slots) * TILE : (s - slots + 1) * TILE]

        low, high = slice(0, TILE), slice(TILE, 2 * TILE)
        context = jnp.zeros((TILE, TILE), F32)
        gq = jnp.zeros((TILE, TILE), F32)
        for s in range(0, slots + c_slots, 2):
            many = [k for k in (s, s + 1) if k < slots + c_slots]
            at = slice(s * TILE, (s + len(many)) * TILE)
            values = jnp.concatenate([turned(k, high) for k in many], axis=1)
            keys = jnp.concatenate([turned(k, low) for k in many], axis=1)
            context = context + dot(values, pd[at, TILE:])
            gq = gq + dot(keys, pd[at, :TILE])
        context = jnp.where(query_slot < len_ref[e], context, 0.0)
        xo[own, :TILE] = context.T.astype(BF)
        xo[own, TILE:] = gq.T.astype(BF)
        return carry

    lax.fori_loop(0, span, bar, 0)
    for j in range(HEADS):
        at = slice(j * block_rows, (j + 1) * block_rows)
        xo_out[at, :] = xo[rows_at(place(j), block_rows), :]
        own_out[at, :] = acc[rows_at(reach * span * TILE + place(j), block_rows), :]
        for t in range(1, reach + 1):
            part = acc[rows_at((reach - t) * span * TILE + place(j), block_rows), :]
            out = back_out[t - 1][j // 2]
            out[j % 2 * block_rows : (j % 2 + 1) * block_rows, :] = part.astype(out.dtype)
    gs_out[...] = gsum[...]


def assemble_kernel(rank_ref, *refs):
    blocks, outs = refs[:HEADS], refs[HEADS:]
    for j, block in enumerate(blocks):
        h = jnp.bitwise_xor(rank_ref[0], j)
        outs[0][:, column(h)] = block[:, :TILE]
        outs[1][:, column(h)] = block[:, TILE:]


def finish_kernel(rank_ref, len_ref, *refs):
    own, backs = refs[0], refs[1:3]
    sums, out, tot = refs[3:-2], refs[-2], refs[-1]
    total = sums[0][...]
    for part in sums[1:]:
        total = total + part[...]
    tot[...] = total
    rows = own.shape[0] // HEADS
    bars = rows // TILE
    slot = lax.broadcasted_iota(jnp.int32, (TILE, 2 * TILE), 0)
    for j in range(HEADS):
        first = jnp.bitwise_xor(rank_ref[0], j) * bars
        for b in range(bars):
            at = slice(j * rows + b * TILE, j * rows + (b + 1) * TILE)
            start = j % 2 * rows + b * TILE
            length = len_ref[first + b]
            count = jnp.full((1, 2 * TILE), length, jnp.int32).astype(F32)
            share = tot[pl.ds(first + b, 1), :] * (1.0 / count)
            value = own[at, :] + backs[j // 2][start : start + TILE, :].astype(F32)
            out[at, :] = (value + jnp.where(slot < length, share, 0.0)).astype(BF)


def weights_kernel(turn, ways, groups, rank_ref, *refs):
    blocks, outs = refs[:HEADS], refs[HEADS:]
    chunk = blocks[0].shape[0] // (ways * groups)
    for j, block in enumerate(blocks):
        h = jnp.bitwise_xor(rank_ref[0], j)
        for s in range(ways):
            for t in range(groups):
                place = jnp.bitwise_xor(rank_ref[3], s) * groups + jnp.bitwise_xor(rank_ref[2], t)
                at = pl.ds(pl.multiple_of(place * chunk, chunk), chunk)
                piece = block[(s * groups + t) * chunk : (s * groups + t + 1) * chunk, :].astype(F32)
                outs[2][at, column(h)] = piece[:, :TILE]
                outs[1][at, column(h)] = piece[:, TILE:]
    if turn:
        for c in range(outs[2].shape[0] // TILE):
            at = slice(c * TILE, (c + 1) * TILE)
            outs[0][:, at] = outs[2][at, :].T
    else:
        outs[0][...] = outs[2][...]


def scatter_sum(part, ways, groups):
    me, group = lax.axis_index("dp"), lax.axis_index("seq") // HEADS
    for axis, size, place, unit in (("dp", ways, me, 1), ("seq", groups, group, HEADS)):
        share = part.shape[0] // size
        total = lax.dynamic_slice_in_dim(part, place * share, share, 0)
        for t in range(1, size):
            send = lax.dynamic_slice_in_dim(part, (place ^ t) * share, share, 0)
            total = total + swap(send.astype(BF), axis, t * unit).astype(F32)
        part = total
    return part.astype(BF)


def spread_groups(share, ways, groups):
    block = jnp.concatenate([share] + [swap(share, "seq", HEADS * t) for t in range(1, groups)], 0)
    return jnp.concatenate([block] + [swap(block, "dp", t) for t in range(1, ways)], 0)


def gathered(block):
    across = swap(block, "seq", 2)
    return [block, swap(block, "seq", 1), across, swap(across, "seq", 1)]


def local(tokens, lengths, w_query, w_key, w_value, w_out, cotangent):
    inputs = tokens[0]
    grad_out = cotangent[0]
    rows, width = inputs.shape
    inner = w_query.shape[1]
    bars = rows // TILE
    span = HEADS * bars
    seq_size = lax.axis_size("seq")
    groups = seq_size // HEADS
    reach = -(-bar_offsets[-1] // span)
    index = lax.axis_index("seq")
    rank = index % HEADS
    group = index // HEADS
    all_length = lengths[0]
    own_length = lax.dynamic_slice_in_dim(all_length, index * bars, bars, 0)
    group_length = lax.dynamic_slice_in_dim(all_length, group * span, span, 0)
    padded = jnp.concatenate([jnp.zeros((reach * span,), jnp.int32), all_length], 0)
    ext_length = lax.dynamic_slice_in_dim(padded, group * span, (reach + 1) * span, 0)
    n_coarse = -(-(groups * span) // TILE) * TILE
    ways = lax.axis_size("dp")
    rank_info = jnp.stack(
        [rank, n_coarse - span - group * span, group, lax.axis_index("dp")]
    ).astype(jnp.int32)

    pair = 2 * TILE
    block = jax.ShapeDtypeStruct((rows, pair), BF)
    wide = jax.ShapeDtypeStruct((rows, pair), F32)
    project = 2 * rows * width * inner

    kv = call(
        kv_kernel,
        [block] * HEADS,
        (rank_info, inputs, w_key, w_value),
        [SM, VM, VM, VM],
        "project_kv",
        2 * project,
        6 << 20,
    )
    kv_own = [kv[0]] + [swap(kv[j], "seq", j) for j in range(1, HEADS)]
    kv_all = [kv_own]
    hop = [jnp.concatenate(kv_own[:2], 0), jnp.concatenate(kv_own[2:], 0)]
    for _ in range(reach):
        hop = [shifted(b, "seq", HEADS) for b in hop]
        kv_all.append(hop)
    qg = call(
        qg_kernel,
        [block] * HEADS,
        (rank_info, own_length, inputs, grad_out, w_query, w_out),
        [SM, SM, VM, VM, VM, VM],
        "project_qg",
        2 * project,
        6 << 20,
    )
    qg = [qg[0]] + [swap(qg[j], "seq", j) for j in range(1, HEADS)]
    summary = call(
        summary_kernel,
        [jax.ShapeDtypeStruct((span, pair), F32)],
        (rank_info, group_length, *kv_own),
        [SM, SM] + [VM] * HEADS,
        "summaries",
        1 << 20,
        1 << 20,
    )[0].astype(BF)
    far = [shifted(summary, "seq", HEADS * t) for t in range(1, groups)]
    padding = jnp.zeros((n_coarse - groups * span, pair), BF)
    sums = jnp.concatenate([padding] + far[::-1] + [summary], 0)

    group_tokens = jnp.concatenate(gathered(inputs), 0)
    group_grad = jnp.concatenate(gathered(grad_out), 0)
    ext_rows = (reach + 1) * span * TILE
    slots = len(bar_offsets) * TILE + n_coarse
    tall = jax.ShapeDtypeStruct((HEADS * rows, pair), BF)
    outs = (
        [tall, jax.ShapeDtypeStruct((HEADS * rows, pair), F32)]
        + [jax.ShapeDtypeStruct((2 * rows, pair), F32)] * (2 * (reach - 1))
        + [jax.ShapeDtypeStruct((2 * rows, pair), BF)] * 2
        + [jax.ShapeDtypeStruct((n_coarse, pair), F32)]
    )

    def kernel(rank_ref, len_ref, *refs):
        take = iter(refs)
        get = lambda n: [next(take) for _ in range(n)]
        qg_in = get(HEADS)
        kv_in = [get(HEADS)] + [get(2) for _ in range(reach)]
        sum_in = next(take)
        xo_out, own_out = get(2)
        back_out = [get(2) for _ in range(reach)]
        gs_out = next(take)
        attention_kernel(
            reach, rank_ref, len_ref, qg_in, kv_in, sum_in,
            (xo_out, own_out, back_out, gs_out), list(take),
        )

    result = call(
        kernel,
        outs,
        (rank_info, ext_length, *qg, *[b for level in kv_all for b in level], sums),
        [SM, SM] + [VM] * (2 * HEADS + 2 * reach + 1),
        "attention",
        16 * slots * TILE * TILE * span,
        16 << 20,
        (
            pltpu.VMEM((span * TILE, pair), BF),
            pltpu.VMEM((ext_rows, pair), BF),
            pltpu.VMEM(((reach + 1) * span, pair, TILE), BF),
            pltpu.VMEM((ext_rows, pair), F32),
            pltpu.VMEM((slots, TILE), F32),
            pltpu.VMEM((slots, TILE), F32),
            pltpu.VMEM((slots, pair), BF),
            pltpu.VMEM((pair, pair), BF),
            pltpu.VMEM((span * TILE, pair), BF),
            pltpu.VMEM((pair, n_coarse), BF),
            pltpu.VMEM((n_coarse, pair), F32),
        ),
    )
    take = iter(result)
    get = lambda n: [next(take) for _ in range(n)]
    xo, own = get(2)
    back = [get(2) for _ in range(reach)]
    gs = next(take)

    carry = back[reach - 1]
    for t in range(reach - 1, -1, -1):
        got = [shifted(b, "seq", -HEADS) for b in carry]
        if t > 0:
            carry = [(b + g.astype(F32)).astype(BF) for b, g in zip(back[t - 1], got)]
    gs_parts = [gs[n_coarse - span :]]
    for t in range(1, groups):
        part = gs[n_coarse - (t + 1) * span : n_coarse - t * span]
        gs_parts.append(shifted(part, "seq", -HEADS * t))

    tn = (((0,), (0,)), ((), ()))
    full = jax.ShapeDtypeStruct((rows, inner), BF)
    square = jax.ShapeDtypeStruct((width, inner), F32)
    crossed = jax.ShapeDtypeStruct((inner, width), F32)

    def owners(packed, name):
        parts = [packed[j * rows : (j + 1) * rows] for j in range(HEADS)]
        parts = [parts[0]] + [swap(parts[j], "seq", j) for j in range(1, HEADS)]
        return call(
            assemble_kernel, [full] * 2, (rank_info, *parts), [SM] + [VM] * HEADS, name, 1 << 20, 2 << 20
        )

    def everywhere(block, turn, name):
        return call(
            functools.partial(weights_kernel, turn, ways, groups),
            [crossed if turn else square, square],
            (rank_info, *gathered(block)),
            [SM] + [VM] * HEADS,
            name,
            1 << 20,
            6 << 20,
            (pltpu.VMEM((width, inner), F32),),
        )

    part = jnp.concatenate(
        [dot(group_grad, xo[:, :TILE], tn), dot(group_tokens, xo[:, TILE:], tn)], 1
    )
    first = spread_groups(scatter_sum(part, ways, groups), ways, groups)
    context, gq = owners(xo, "join_q")
    mixed = dot(context, w_out).astype(BF)
    got, first = lax.optimization_barrier((got, first))
    gkv = call(
        finish_kernel,
        [tall],
        (rank_info, group_length, own, *got, *gs_parts),
        [SM, SM] + [VM] * (3 + groups),
        "finish_kv",
        1 << 20,
        4 << 20,
        (pltpu.VMEM((span, pair), F32),),
    )[0]
    second = spread_groups(
        scatter_sum(dot(group_tokens, gkv, tn), ways, groups), ways, groups
    )
    gk, gv = owners(gkv, "join_kv")
    grad_in = dot(gq, w_query, NT) + dot(gk, w_key, NT) + dot(gv, w_value, NT)
    grad_o, grad_q = everywhere(first, True, "weights_oq")
    grad_k, grad_v = everywhere(second, False, "weights_kv")
    return (
        mixed[None],
        grad_in.astype(BF)[None],
        grad_q,
        grad_k,
        grad_v,
        grad_o,
    )


def solution(mesh):
    placed = (P("dp", "seq", None), P("dp", None), P(), P(), P(), P(), P("dp", "seq", None))
    return jax.shard_map(
        local,
        mesh=mesh,
        in_specs=placed,
        out_specs=(P("dp", "seq", None), P("dp", "seq", None), P(), P(), P(), P()),
        check_vma=False,
    )
```
